16 devices in a mesh: rep: 1, dp: 16 (over x, y, z, core).
Axes of the slice: x: 2, y: 2, z: 2, core: 2. Of those that a mesh axis runs over, the one named last changes fastest.
Arguments:
- x: bfloat16 [16, 2048, 1024], P(('rep', 'dp'))
- dy: bfloat16 [16, 2048, 1024], P(('rep', 'dp'))
- wq: bfloat16 [2, 1024, 1024], P(None, 'dp')
- wk: bfloat16 [2, 1024, 1024], P(None, 'dp')
- wv: bfloat16 [2, 1024, 1024], P(None, 'dp')
- wo: bfloat16 [2, 1024, 1024], P(None, 'dp')
- w_gate: bfloat16 [2, 1024, 4096], P(None, 'dp')
- w_up: bfloat16 [2, 1024, 4096], P(None, 'dp')
- w_down: bfloat16 [2, 4096, 1024], P(None, 'dp')
Outputs:
- output 1: bfloat16 [16, 2048, 1024], P(('rep', 'dp'))
- output 2: bfloat16 [2, 1024, 1024], P('rep', 'dp')
- output 3: bfloat16 [2, 1024, 1024], P('rep', 'dp')
- output 4: bfloat16 [2, 1024, 1024], P('rep', 'dp')
- output 5: bfloat16 [2, 1024, 1024], P('rep', 'dp')
- output 6: bfloat16 [2, 1024, 4096], P('rep', 'dp')
- output 7: bfloat16 [2, 1024, 4096], P('rep', 'dp')
- output 8: bfloat16 [2, 4096, 1024], P('rep', 'dp')
All inputs are finite; a program needn't handle non-finite values.
Results may differ from the reference program's by a relative error of at most 0.0305.
Values are sent between devices in bfloat16 or wider.
A program may use at most 2 GiB of HBM per device.

```python
import jax
import jax.numpy as jnp
from jax import lax

SEQUENCES = 16
TOKENS = 2048
D = 1024
HEADS = 4
KV_HEADS = 4
HEAD = 256
FF = 4096
LAYERS = 2
THETA = 10000
NAMES = ("wq", "wk", "wv", "wo", "w_gate", "w_up", "w_down")
SHAPES = {
    "wq": (LAYERS, D, HEADS * HEAD),
    "wk": (LAYERS, D, KV_HEADS * HEAD),
    "wv": (LAYERS, D, KV_HEADS * HEAD),
    "wo": (LAYERS, HEADS * HEAD, D),
    "w_gate": (LAYERS, D, FF),
    "w_up": (LAYERS, D, FF),
    "w_down": (LAYERS, FF, D),
}


def bump(key, n, height):
    away = (jnp.arange(n, dtype=jnp.int32) - jax.random.randint(key, (), 0, n, jnp.int32)) % n
    return jnp.where(away < n // 8, height, 1.0)


def together(key, own, strength):
    shared = jax.random.normal(key, own.shape[1:], jnp.float32)
    return (own + strength * shared) * lax.rsqrt(1 + strength * strength)


def setup_inputs(seed: int = 0, part: int = 0) -> dict:
    kx, kdy, ka, kb, kz, kf, kh, kl, *keys = jax.random.split(jax.random.key(seed), 8 + 3 * len(NAMES))
    kx, kdy, ka, kb = (jax.random.fold_in(k, part) for k in (kx, kdy, ka, kb))
    kw, km, kv = (keys[i::3] for i in range(3))
    shape = (SEQUENCES, TOKENS, D)
    much_x, much_dy = jax.random.uniform(kz, (2,), jnp.float32, 0.0, 1.0)
    loud = 2.0 ** jax.random.uniform(jax.random.fold_in(kz, 1), (), jnp.float32, -1.0, 2.0)
    layers = 2.0 ** jax.random.uniform(kl, (LAYERS, 1, 1), jnp.float32, -1.0, 1.0)
    times = {"wq": 1.0, "wk": 1.0, "wv": 2.0, "wo": layers, "w_gate": 1.0, "w_up": bump(kh, FF, 4.0), "w_down": layers}
    x = together(ka, jax.random.normal(kx, shape, jnp.float32), much_x) * bump(kf, D, 4.0)
    dy = together(kb, jax.random.normal(kdy, shape, jnp.float32), much_dy)
    drawn = {"x": x.astype(jnp.bfloat16), "dy": (loud * dy * (SEQUENCES * TOKENS) ** -0.5).astype(jnp.bfloat16)}
    for key, name in zip(kw, NAMES, strict=True):
        drawn[name] = (jax.random.normal(key, SHAPES[name], jnp.float32) * SHAPES[name][1] ** -0.5 * times[name]).astype(jnp.bfloat16)
    return drawn


def matmul(a, w):
    return jnp.dot(a, w, preferred_element_type=jnp.float32).astype(jnp.bfloat16)


def normed(h):
    wide = h.astype(jnp.float32)
    scale = lax.rsqrt(jnp.mean(wide**2, -1, keepdims=True) + 1e-6)
    return (wide * scale).astype(jnp.bfloat16)


def turned(t, theta):
    half = t.shape[-1] // 2
    angle = jnp.arange(t.shape[0], dtype=jnp.float32)[:, None] * theta ** (-jnp.arange(half, dtype=jnp.float32) / half)
    cos, sin = jnp.cos(angle)[:, None], jnp.sin(angle)[:, None]
    a, b = t[..., :half].astype(jnp.float32), t[..., half:].astype(jnp.float32)
    return jnp.concatenate([a * cos - b * sin, b * cos + a * sin], -1).astype(jnp.bfloat16)


def seen_by(q, k, v):
    tokens, kv = q.shape[0], k.shape[1]
    q = q.reshape(tokens, kv, -1, q.shape[-1])
    scores = jnp.einsum("tgsd,ugd->gstu", q.astype(jnp.float32), k.astype(jnp.float32)) * q.shape[-1] ** -0.5
    place = jnp.arange(tokens)
    weights = jax.nn.softmax(jnp.where(place[:, None] >= place, scores, -jnp.inf), -1).astype(jnp.bfloat16)
    return jnp.einsum("gstu,ugd->tgsd", weights.astype(jnp.float32), v.astype(jnp.float32)).astype(jnp.bfloat16).reshape(tokens, -1)


def layer(h, w):
    a = normed(h)
    q, k = (turned(matmul(a, w[name]).reshape(h.shape[0], -1, HEAD), THETA) for name in ("wq", "wk"))
    h = h + matmul(seen_by(q, k, matmul(a, w["wv"]).reshape(h.shape[0], -1, HEAD)), w["wo"])
    b = normed(h)
    gate = jnp.dot(b, w["w_gate"], preferred_element_type=jnp.float32)
    up = jnp.dot(b, w["w_up"], preferred_element_type=jnp.float32)
    return h + matmul((jax.nn.silu(gate) * up).astype(jnp.bfloat16), w["w_down"])


def stack(weights, h):
    return lax.scan(lambda h, w: (layer(h, w), None), h, weights)[0]


def reference(x, dy, wq, wk, wv, wo, w_gate, w_up, w_down):
    weights = dict(zip(NAMES, (wq, wk, wv, wo, w_gate, w_up, w_down), strict=True))

    def take(so_far, sequence):
        h, by_y = sequence
        _, back = jax.vjp(stack, weights, h)
        by_weights, by_h = back(by_y)
        return jax.tree.map(lambda total, term: total + term.astype(jnp.float32), so_far, by_weights), by_h

    none_yet = {name: jnp.zeros(w.shape, jnp.float32) for name, w in weights.items()}
    by_weights, by_x = lax.scan(take, none_yet, (x, dy))
    return (by_x, *(by_weights[name].astype(jnp.bfloat16) for name in NAMES))
```

```python
import functools

import jax
import jax.numpy as jnp
from jax import lax
from jax.experimental import pallas as pl
from jax.experimental.pallas import tpu as pltpu
from jax.sharding import PartitionSpec as P

NEG = -1e30
HIDDEN = 2 * NEG
LOG2E = 1.4426950408889634
VMEM = 56 * 2**20
STRIP = 512
HEAD = 256
HALF = HEAD // 2
THETA = 10000
BF, F32 = jnp.bfloat16, jnp.float32

SLOW = (1,)


def _dot(a, b, ca, cb):
    return lax.dot_general(a, b, (((ca,), (cb,)), ((), ())), preferred_element_type=F32)


def _turn(t, cos, sin):
    a, b = t[:, :HALF].astype(F32), t[:, HALF:].astype(F32)
    return jnp.concatenate([a * cos - b * sin, b * cos + a * sin], 1).astype(BF)


def _turn_back(t, cos, sin):
    a, b = t[:, :HALF].astype(F32), t[:, HALF:].astype(F32)
    return jnp.concatenate([a * cos + b * sin, b * cos - a * sin], 1).astype(BF)


def _attend_kernel(cq_ref, sq_ref, ck_ref, sk_ref, q_ref, k_ref, v_ref, o_ref, lse_ref, qr_ref, kr_ref, top_s, mix_s, gap_s, *, heads, bq, bk):
    iq = pl.program_id(0)
    sk = k_ref.shape[0]
    scale = HEAD**-0.5
    e = scale * LOG2E
    pieces = [(i, at) for i in range(heads) for at in range(0, bq, STRIP)]
    head = lambda i: slice(i * HEAD, (i + 1) * HEAD)

    @pl.when(iq == 0)
    def _():
        gap_s[...] = lax.broadcasted_iota(jnp.int32, (bk, STRIP), 1) - lax.broadcasted_iota(jnp.int32, (bk, STRIP), 0)

        def rotate(n, _):
            at = pl.ds(n * 256, 256)
            for i in range(heads):
                kr_ref[at, head(i)] = _turn(k_ref[at, head(i)], ck_ref[at, :], sk_ref[at, :])

        lax.fori_loop(0, sk // 256, rotate, None)

    for i in range(heads):
        qr_ref[:, head(i)] = _turn(q_ref[:, head(i)], cq_ref[...], sq_ref[...])
    top_s[...] = jnp.full_like(top_s, NEG)
    mix_s[...] = jnp.zeros_like(mix_s)
    ones = jnp.ones((8, bk), BF)

    def block(j, pieces, diagonal):
        here = pl.ds(j * bk, bk)
        scores = [_dot(kr_ref[here, head(i)], qr_ref[at : at + STRIP, head(i)], 1, 1) for i, at in pieces]
        ok = gap_s[...] >= 0
        weights, keeps = [], []
        for (i, at), s in zip(pieces, scores):
            if at == diagonal:
                s = jnp.where(ok, s, HIDDEN)
            old = top_s[i : i + 1, at : at + STRIP]
            top = jnp.maximum(old, s.max(axis=0, keepdims=True))
            top_s[i : i + 1, at : at + STRIP] = top
            weights.append(jnp.exp2((s - top) * e).astype(BF))
            keeps.append(jnp.exp2((old - top) * e))
        for (i, at), p, keep in zip(pieces, weights, keeps):
            values = jnp.concatenate([v_ref[here, head(i)].T, ones], axis=0)
            mix_s[i, :, at : at + STRIP] = mix_s[i, :, at : at + STRIP] * keep + _dot(values, p, 1, 0)

    whole = iq * (bq // bk)
    lax.fori_loop(0, whole, lambda j, _: block(j, pieces, None), None)
    for at in range(0, bq, bk):
        block(whole + at // bk, [p for p in pieces if p[1] >= at], at)
    for i in range(heads):
        top, total = top_s[i : i + 1, :], mix_s[i, HEAD : HEAD + 1, :]
        o_ref[:, head(i)] = (mix_s[i, :HEAD, :] * (1 / total)).T.astype(BF)
        lse_ref[i : i + 1, :] = top * scale + jnp.log(total)


def attend(q, k, v, cos, sin):
    s, width = q.shape
    heads, bq, bk = width // HEAD, 1024, STRIP
    rows = lambda w: pl.BlockSpec((bq, w), lambda i: (i, 0))
    full = lambda w: pl.BlockSpec((s, w), lambda i: (0, 0))
    return pl.pallas_call(
        functools.partial(_attend_kernel, heads=heads, bq=bq, bk=bk),
        grid=(s // bq,),
        in_specs=[rows(HALF), rows(HALF), full(HALF), full(HALF), rows(width), full(width), full(width)],
        out_specs=[rows(width), pl.BlockSpec((heads, bq), lambda i: (0, i)), rows(width), full(width)],
        scratch_shapes=[pltpu.VMEM((heads, bq), F32), pltpu.VMEM((heads, HEAD + 8, bq), F32), pltpu.VMEM((bk, STRIP), jnp.int32)],
        out_shape=[jax.ShapeDtypeStruct((s, width), BF), jax.ShapeDtypeStruct((heads, s), F32), jax.ShapeDtypeStruct((s, width), BF),
                   jax.ShapeDtypeStruct((s, width), BF)],
        compiler_params=pltpu.CompilerParams(dimension_semantics=("arbitrary",), vmem_limit_bytes=VMEM),
        cost_estimate=pl.CostEstimate(flops=6 * s * s * width, transcendentals=heads * s * s, bytes_accessed=14 * s * width),
    )(cos, sin, cos, sin, q, k, v)


def _attend_bwd_kernel(cq_ref, sq_ref, ck_ref, sk_ref, q_ref, k_ref, v_ref, o_ref, do_ref, lse_ref, dq_ref, dk_ref, dv_ref, dq_s, dk_s, dv_s, gap_s,
                       *, heads, bq, bk):
    iq = pl.program_id(1)
    sk = k_ref.shape[0]
    scale = HEAD**-0.5
    e = scale * LOG2E
    pieces = [(i, at) for i in range(heads) for at in range(0, bq, STRIP)]
    head = lambda i: slice(i * HEAD, (i + 1) * HEAD)

    @pl.when(iq == 0)
    def _():
        gap_s[...] = lax.broadcasted_iota(jnp.int32, (bk, STRIP), 1) - lax.broadcasted_iota(jnp.int32, (bk, STRIP), 0)
        dk_s[...] = jnp.zeros_like(dk_s)
        dv_s[...] = jnp.zeros_like(dv_s)

    dq_s[...] = jnp.zeros_like(dq_s)
    lses = [lse_ref[0, i : i + 1, :] * LOG2E for i in range(heads)]
    deltas = [(do_ref[:, head(i)].astype(F32) * o_ref[:, head(i)].astype(F32)).T.sum(axis=0, keepdims=True) for i in range(heads)]

    def block(j, pieces, diagonal):
        here = pl.ds(j * bk, bk)
        qs = [q_ref[at : at + STRIP, head(i)] for i, at in pieces]
        dos = [do_ref[at : at + STRIP, head(i)] for i, at in pieces]
        scores = [_dot(k_ref[here, head(i)], x, 1, 1) for (i, _), x in zip(pieces, qs)]
        dps = [_dot(v_ref[here, head(i)], x, 1, 1) for (i, _), x in zip(pieces, dos)]
        ok = gap_s[...] >= 0
        for n, (i, at) in enumerate(pieces):
            p = jnp.exp2(scores[n] * e - lses[i][:, at : at + STRIP])
            if at == diagonal:
                p = jnp.where(ok, p, 0.0)
            ds = (p * (dps[n] - deltas[i][:, at : at + STRIP])).astype(BF)
            dv_s[i, here, :] += _dot(p.astype(BF), dos[n], 1, 0)
            dk_s[i, here, :] += _dot(ds, qs[n], 1, 0)
            dq_s[i, :, at : at + STRIP] += _dot(k_ref[here, head(i)].T, ds, 1, 0)

    whole = iq * (bq // bk)
    lax.fori_loop(0, whole, lambda j, _: block(j, pieces, None), None)
    for at in range(0, bq, bk):
        block(whole + at // bk, [p for p in pieces if p[1] >= at], at)
    for i in range(heads):
        dq_ref[:, head(i)] = _turn_back((dq_s[i] * scale).T.astype(BF), cq_ref[...], sq_ref[...])

    @pl.when(iq == pl.num_programs(1) - 1)
    def _():
        def finish(n, _):
            at = pl.ds(n * 256, 256)
            for i in range(heads):
                dk_ref[at, head(i)] = _turn_back((dk_s[i, at, :] * scale).astype(BF), ck_ref[at, :], sk_ref[at, :])
                dv_ref[at, head(i)] = dv_s[i, at, :].astype(BF)

        lax.fori_loop(0, sk // 256, finish, None)


def attend_bwd(q, k, v, o, do, lse, cos, sin):
    s, width = q.shape
    heads, bq, bk = 2, 1024, STRIP
    w = heads * HEAD
    lse = lse.reshape(width // w, heads, s)
    rows = pl.BlockSpec((bq, w), lambda h, i: (i, h))
    full = pl.BlockSpec((s, w), lambda h, i: (0, h))
    table, tables = pl.BlockSpec((bq, HALF), lambda h, i: (i, 0)), pl.BlockSpec((s, HALF), lambda h, i: (0, 0), pipeline_mode=pl.Buffered(1))
    like = jax.ShapeDtypeStruct((s, width), BF)
    return pl.pallas_call(
        functools.partial(_attend_bwd_kernel, heads=heads, bq=bq, bk=bk),
        grid=(width // w, s // bq),
        in_specs=[table, table, tables, tables, rows, full, full, rows, rows, pl.BlockSpec((1, heads, bq), lambda h, i: (h, 0, i))],
        out_specs=[rows, full, full],
        scratch_shapes=[pltpu.VMEM((heads, HEAD, bq), F32), pltpu.VMEM((heads, s, HEAD), F32), pltpu.VMEM((heads, s, HEAD), F32),
                        pltpu.VMEM((bk, STRIP), jnp.int32)],
        out_shape=[like, like, like],
        compiler_params=pltpu.CompilerParams(dimension_semantics=("arbitrary", "arbitrary"), vmem_limit_bytes=63 * 2**20),
        cost_estimate=pl.CostEstimate(flops=12 * s * s * width, transcendentals=width // HEAD * s * s, bytes_accessed=16 * s * width),
    )(cos, sin, cos, sin, q, k, v, o, do, lse)


def matmul(a, w):
    return jnp.dot(a, w, preferred_element_type=F32).astype(BF)


def scale_of(wide):
    return lax.rsqrt(jnp.mean(wide**2, -1, keepdims=True) + 1e-6)


def normed(h):
    wide = h.astype(F32)
    return (wide * scale_of(wide)).astype(BF)


def norm_bwd(h, dn, dh):
    wide, dn = h.astype(F32), dn.astype(F32)
    s = scale_of(wide)
    mean = jnp.mean(wide * dn, -1, keepdims=True)
    return (dh.astype(F32) + s * (dn - wide * (s * s * mean))).astype(BF)


ROWS = 256
TILE = 512


def _strips(s):
    return [slice(at, at + ROWS) for at in range(0, s, ROWS)]


def _slopes(gate, up, dact):
    sig = jax.nn.sigmoid(gate)
    dact = dact.astype(BF).astype(F32)
    swish = gate * sig
    return (dact * up * (sig + swish * (1 - sig))).astype(BF), (dact * swish).astype(BF)


def _up_kernel(b_ref, wg_ref, wu_ref, gate_ref, up_ref, act_ref):
    for r in _strips(b_ref.shape[0]):
        gate, up = _dot(b_ref[r, :], wg_ref[...], 1, 0), _dot(b_ref[r, :], wu_ref[...], 1, 0)
        gate_ref[r, :] = gate
        up_ref[r, :] = up
        act_ref[r, :] = (gate * jax.nn.sigmoid(gate) * up).astype(BF)


def _slope_kernel(gate_ref, up_ref, dh_ref, wd_ref, dgate_ref, dup_ref):
    for r in _strips(dh_ref.shape[0]):
        dact = _dot(dh_ref[r, :], wd_ref[...], 1, 1)
        dgate_ref[r, :], dup_ref[r, :] = _slopes(gate_ref[r, :], up_ref[r, :], dact)


def _both_kernel(b_ref, wg_ref, wu_ref, dact_ref, act_ref, dgate_ref, dup_ref):
    for r in _strips(b_ref.shape[0]):
        gate, up = _dot(b_ref[r, :], wg_ref[...], 1, 0), _dot(b_ref[r, :], wu_ref[...], 1, 0)
        dact = dact_ref[r, :]
        act_ref[r, :] = (gate * jax.nn.sigmoid(gate) * up).astype(BF)
        dgate_ref[r, :], dup_ref[r, :] = _slopes(gate, up, dact)


def _back_kernel(*refs):
    pairs, (h_ref, dh_ref, out_ref) = refs[:-3], refs[-3:]
    for r in _strips(h_ref.shape[0]):
        dn = sum(_dot(g[r, :], w[...], 1, 1) for g, w in zip(pairs[::2], pairs[1::2]))
        out_ref[r, :] = norm_bwd(h_ref[r, :], dn.astype(BF), dh_ref[r, :])


def _ffn(kernel, arrays, kinds, outs, scratch, flops, exps):
    def spec(kind, a):
        if kind == "full":
            return pl.BlockSpec(a.shape, lambda n: (0, 0))
        if kind == "cols":
            return pl.BlockSpec((a.shape[0], TILE), lambda n: (0, n))
        number, way = kind
        if way == "out":
            return pl.BlockSpec((None, TILE, a.shape[2]), lambda n: (number, n, 0))
        return pl.BlockSpec((None, a.shape[1], TILE), lambda n: (number, 0, n))

    hidden = max(a.shape[-1] if kind == "cols" or kind[1] == "in" else 0 for kind, a in zip(kinds, arrays))
    return pl.pallas_call(
        kernel,
        grid=(hidden // TILE,),
        in_specs=[spec(kind, a) for kind, a in zip(kinds, arrays)],
        out_specs=[spec(kind, o) for kind, o in outs],
        out_shape=[o for _, o in outs],
        scratch_shapes=scratch,
        compiler_params=pltpu.CompilerParams(dimension_semantics=("arbitrary",), vmem_limit_bytes=VMEM),
        cost_estimate=pl.CostEstimate(flops=flops, transcendentals=exps, bytes_accessed=sum(o.size * o.dtype.itemsize for _, o in outs) * 2),
    )(*arrays)


def ffn_up(b, wide):
    s, d, f = *b.shape, wide.shape[2]
    like = lambda t: ("cols", jax.ShapeDtypeStruct((s, f), t))
    return _ffn(_up_kernel, [b, wide, wide], ["full", (0, "in"), (1, "in")], [like(F32), like(F32), like(BF)], [], 4 * s * d * f, s * f)


def ffn_slope(gate, up, dh, down, number):
    s, d, f = *dh.shape, gate.shape[1]
    like = ("cols", jax.ShapeDtypeStruct((s, f), BF))
    return _ffn(_slope_kernel, [gate, up, dh, down], ["cols", "cols", "full", (number, "out")], [like, like], [], 2 * s * d * f, s * f)


def ffn_both(b, wide, dact):
    s, d, f = *b.shape, wide.shape[2]
    like = ("cols", jax.ShapeDtypeStruct((s, f), BF))
    return _ffn(_both_kernel, [b, wide, wide, dact], ["full", (0, "in"), (1, "in"), "cols"], [like] * 3, [], 4 * s * d * f, s * f)


def norm_back(pairs, h, dh):
    s, d = h.shape
    rows = lambda a: pl.BlockSpec((2 * ROWS, a.shape[1]), lambda i: (i, 0))
    arrays, specs = [], []
    for g, (stack, number) in pairs:
        arrays += [g, stack]
        specs += [rows(g), pl.BlockSpec((None, *stack.shape[1:]), lambda i, number=number: (number, 0, 0), pipeline_mode=pl.Buffered(1))]
    flops = sum(2 * s * d * g.shape[1] for g, _ in pairs)
    return pl.pallas_call(
        _back_kernel,
        grid=(s // (2 * ROWS),),
        in_specs=[*specs, rows(h), rows(dh)],
        out_specs=rows(h),
        out_shape=jax.ShapeDtypeStruct((s, d), BF),
        compiler_params=pltpu.CompilerParams(dimension_semantics=("arbitrary",), vmem_limit_bytes=VMEM),
        cost_estimate=pl.CostEstimate(flops=flops, transcendentals=0, bytes_accessed=6 * s * d + flops // d),
    )(*arrays, h, dh)


def solution(mesh):
    n = mesh.shape["dp"]

    def gather(blocks):
        return lax.all_gather(jnp.stack(blocks), "dp", axis=1, tiled=True)

    class Scatter:
        def __init__(self, *dws):
            rows = dws[0].shape[0] // n
            self.own = [dw.reshape(n // 2, 2, rows, dw.shape[1]) for dw in dws]
            self.widths = [dw.shape[1] for dw in dws]
            self.stage, self.got, self.half = 0, None, None

        def term(self, chip):
            core = lax.axis_index("dp") & 1
            own = [lax.dynamic_slice(o, (chip, core, 0, 0), (1, 1, *o.shape[2:]))[0, 0] for o in self.own]
            got = lax.dynamic_index_in_dim(self.half, chip, 0, False)
            return jnp.concatenate(own, -1).astype(F32) + got.astype(F32)

        def outs(self):
            me = lax.axis_index("dp")
            if self.stage == 0:
                return [jnp.concatenate([lax.dynamic_index_in_dim(o, 1 - (me & 1), 1, False) for o in self.own], -1)]
            return [self.term((me >> 1) ^ m).astype(BF) for m in range(1, n // 2)]

        def send(self, outs):
            masks = [1] if self.stage == 0 else [2 * m for m in range(1, n // 2)]
            self.got = [lax.ppermute(o, "dp", [(i, i ^ mask) for i in range(n)]) for o, mask in zip(outs, masks)]

        def take(self):
            if self.stage == 0:
                self.half = self.got[0]
            else:
                self.others = self.got
            self.got = None
            self.stage += 1

        def result(self):
            while self.stage < 2:
                if self.got is None:
                    self.send(self.outs())
                self.take()
            total = self.term(lax.axis_index("dp") >> 1)
            for o in self.others:
                total += o.astype(F32)
            total, out, at = total.astype(BF), [], 0
            for w in self.widths:
                out.append(total[:, at : at + w])
                at += w
            return out

    class Offloaded:
        def __init__(self, blocks):
            block = jnp.stack(blocks) if len(blocks) > 1 else blocks[0]
            self.mib = block.size * 2 / 2**20
            self.got = lax.psum_scatter(block, "dp", scatter_dimension=block.ndim - 2, tiled=True)

        def parts(self):
            return list(self.got) if self.got.ndim == 3 else [self.got]

    class Line:
        def __init__(self):
            self.now, self.free, self.active, self.last = 0.0, [0.0, 0.0], [], None
            self.queue, self.queue_free = [], 0.0

        def step(self, took, *operands):
            self.now += took
            due = [s for s in self.active if s.got is not None and s.ready <= self.now]
            back = [o for o in self.queue if o.ready <= self.now]
            self.queue = [o for o in self.queue if o not in back]
            operands, _, gots, whole = lax.optimization_barrier((operands, self.last, [s.got for s in due], [o.got for o in back]))
            for o, got in zip(back, whole):
                o.got = got
            for s, got in zip(due, gots):
                s.got = got
                s.take()
            idle = [s for s in self.active if s.got is None and s.stage < 2]
            outs = [s.outs() for s in idle]
            operands, outs = lax.optimization_barrier((operands, outs))
            for s, out in zip(idle, outs):
                s.send(out)
                mib = out[0].size * 2 / 2**20
                begin = max(self.now, self.free[s.stage])
                s.ready = begin + (94 * mib if s.stage else 2.1 * mib) + 4
                self.free[s.stage] = s.ready
            return operands if len(operands) > 1 else operands[0]

        def flush(self):
            late = [s for s in self.active if s.got is not None]
            self.last, gots = lax.optimization_barrier((self.last, [s.got for s in late]))
            for s, got in zip(late, gots):
                s.got = got
            return self.last

        def done(self, result):
            self.last = result
            return result

        def scatter(self, *dws):
            self.active.append(Scatter(*dws))
            return self.active[-1]

        def offload(self, *blocks):
            o = Offloaded(blocks)
            o.ready = self.queue_free = max(self.now, self.queue_free) + 75 + 6.2 * o.mib
            self.queue.append(o)
            return o

    def step(x, dy, wq, wk, wv, wo, w_gate, w_up, w_down):
        h, dh = x[0], dy[0]
        s = h.shape[0]
        angle = jnp.arange(s, dtype=F32)[:, None] * THETA ** (-jnp.arange(HALF, dtype=F32) / HALF)
        cos, sin = jnp.cos(angle), jnp.sin(angle)

        small = [None, None]
        wide = [None, None]
        small[0] = gather([wq[0], wk[0], wv[0], wo[0]])
        wide[0] = gather([w_gate[0], w_up[0]])
        down = gather([w_down[0], w_down[1]])
        small[1] = gather([wq[1], wk[1], wv[1], wo[1]])
        wide[1] = gather([w_gate[1], w_up[1]])

        kept = []
        for l in range(2):
            a = normed(h)
            q, k, v = (matmul(a, small[l][i]) for i in range(3))
            o, lse, q, k = attend(q, k, v, cos, sin)
            h2 = h + matmul(o, small[l][3])
            b = normed(h2)
            if l == 0:
                gate, up, act = ffn_up(b, wide[l])
                kept.append((h, a, q, k, v, o, lse, h2, b, gate, up, act))
                h = h2 + matmul(act, down[l])
                h, dh_in = lax.optimization_barrier((h, dh))
                dact = matmul(dh_in, down[1].T)
                h, dact = lax.optimization_barrier((h, dact))
        act, dgate, dup = ffn_both(b, wide[1], dact)
        kept.append((h, a, q, k, v, o, lse, h2, b, None, None, act))

        grads = [None, None]
        line = Line()
        for l in (1, 0):
            h, a, q, k, v, o, lse, h2, b, gate, up, act = kept[l]
            big = line.offload if l in SLOW else line.scatter
            if l == 0:
                dh_in = line.step(6, dh)
                dgate, dup = ffn_slope(gate, up, dh_in, down, 0)
            line.done((dgate, dup))
            act, dh_in = line.step(40, act, dh)
            g_down = big(line.done(matmul(act.T, dh_in)))
            b1, dgate = line.step(26, b, dgate)
            g_gate = big(line.done(matmul(b1.T, dgate)))
            b1, dup = line.step(21, b, dup)
            g_up = big(line.done(matmul(b1.T, dup)))
            dgate = line.step(21, dgate)
            dh2 = line.done(norm_back([(dgate, (wide[l], 0)), (dup, (wide[l], 1))], h2, dh))
            dh_in = line.step(45, dh2)
            do = line.done(matmul(dh_in, small[l][3].T))
            do = line.step(8, do)
            dq, dk, dv = line.done(attend_bwd(q, k, v, o, do, lse, cos, sin))
            a1, dq = line.step(47, a, dq)
            g_q = line.done(matmul(a1.T, dq))
            a1, dk = line.step(6, a, dk)
            g_k = line.done(matmul(a1.T, dk))
            if l not in SLOW:
                few = [line.scatter(g_q, g_k)]
            a1, dv = line.step(6, a, dv)
            g_v = line.done(matmul(a1.T, dv))
            o1, dh_in = line.step(6, o, dh2)
            g_o = line.done(matmul(o1.T, dh_in))
            if l in SLOW:
                few = [line.offload(g_q, g_k, g_v, g_o)]
                dq = line.step(6, dq)
            else:
                few.append(line.scatter(g_v, g_o))
                dq = line.step(6, dq)
                dq = line.step(9, dq)
            dh = line.done(norm_back([(dq, (small[l], 0)), (dk, (small[l], 1)), (dv, (small[l], 2))], h, dh2))
            line.now += 25
            grads[l] = [*few, g_gate, g_up, g_down]
        dh = line.flush()
        grads = [[t for g in gs for t in (g.result() if isinstance(g, Scatter) else g.parts())] for gs in grads]
        return (dh[None], *(jnp.stack([grads[0][i], grads[1][i]]) for i in range(7)))

    states, cut = P(("rep", "dp"), None, None), P(None, "dp", None)
    return jax.shard_map(
        step,
        mesh=mesh,
        in_specs=(states, states) + (cut,) * 7,
        out_specs=(states,) + (P("rep", "dp", None),) * 7,
        check_vma=False,
    )
```

```python
import functools

import jax
import jax.numpy as jnp
from jax import lax
from jax.experimental import pallas as pl
from jax.experimental.pallas import tpu as pltpu
from jax.sharding import PartitionSpec as P

NEG = -1e30
HIDDEN = 2 * NEG
LOG2E = 1.4426950408889634
VMEM = 56 * 2**20
STRIP = 512
HEAD = 256
HALF = HEAD // 2
THETA = 10000
BF, F32 = jnp.bfloat16, jnp.float32

SLOW = (1,)


def _dot(a, b, ca, cb):
    return lax.dot_general(a, b, (((ca,), (cb,)), ((), ())), preferred_element_type=F32)


def _turn(t, cos, sin):
    a, b = t[:, :HALF].astype(F32), t[:, HALF:].astype(F32)
    return jnp.concatenate([a * cos - b * sin, b * cos + a * sin], 1).astype(BF)


def _turn_back(t, cos, sin):
    a, b = t[:, :HALF].astype(F32), t[:, HALF:].astype(F32)
    return jnp.concatenate([a * cos + b * sin, b * cos - a * sin], 1).astype(BF)


def _attend_kernel(cq_ref, sq_ref, ck_ref, sk_ref, q_ref, k_ref, v_ref, o_ref, lse_ref, qr_ref, kr_ref, top_s, mix_s, gap_s, *, heads, bq, bk):
    iq = pl.program_id(0)
    sk = k_ref.shape[0]
    scale = HEAD**-0.5
    e = scale * LOG2E
    pieces = [(i, at) for i in range(heads) for at in range(0, bq, STRIP)]
    head = lambda i: slice(i * HEAD, (i + 1) * HEAD)

    @pl.when(iq == 0)
    def _():
        gap_s[...] = lax.broadcasted_iota(jnp.int32, (bk, STRIP), 1) - lax.broadcasted_iota(jnp.int32, (bk, STRIP), 0)

        def rotate(n, _):
            at = pl.ds(n * 256, 256)
            for i in range(heads):
                kr_ref[at, head(i)] = _turn(k_ref[at, head(i)], ck_ref[at, :], sk_ref[at, :])

        lax.fori_loop(0, sk // 256, rotate, None)

    for i in range(heads):
        qr_ref[:, head(i)] = _turn(q_ref[:, head(i)], cq_ref[...], sq_ref[...])
    top_s[...] = jnp.full_like(top_s, NEG)
    mix_s[...] = jnp.zeros_like(mix_s)
    ones = jnp.ones((8, bk), BF)

    def block(j, pieces, diagonal):
        here = pl.ds(j * bk, bk)
        scores = [_dot(kr_ref[here, head(i)], qr_ref[at : at + STRIP, head(i)], 1, 1) for i, at in pieces]
        ok = gap_s[...] >= 0
        weights, keeps = [], []
        for (i, at), s in zip(pieces, scores):
            if at == diagonal:
                s = jnp.where(ok, s, HIDDEN)
            old = top_s[i : i + 1, at : at + STRIP]
            top = jnp.maximum(old, s.max(axis=0, keepdims=True))
            top_s[i : i + 1, at : at + STRIP] = top
            weights.append(jnp.exp2((s - top) * e).astype(BF))
            keeps.append(jnp.exp2((old - top) * e))
        for (i, at), p, keep in zip(pieces, weights, keeps):
            values = jnp.concatenate([v_ref[here, head(i)].T, ones], axis=0)
            mix_s[i, :, at : at + STRIP] = mix_s[i, :, at : at + STRIP] * keep + _dot(values, p, 1, 0)

    whole = iq * (bq // bk)
    lax.fori_loop(0, whole, lambda j, _: block(j, pieces, None), None)
    for at in range(0, bq, bk):
        block(whole + at // bk, [p for p in pieces if p[1] >= at], at)
    for i in range(heads):
        top, total = top_s[i : i + 1, :], mix_s[i, HEAD : HEAD + 1, :]
        o_ref[:, head(i)] = (mix_s[i, :HEAD, :] * (1 / total)).T.astype(BF)
        lse_ref[i : i + 1, :] = top * scale + jnp.log(total)


def attend(q, k, v, cos, sin):
    s, width = q.shape
    heads, bq, bk = width // HEAD, 1024, STRIP
    rows = lambda w: pl.BlockSpec((bq, w), lambda i: (i, 0))
    full = lambda w: pl.BlockSpec((s, w), lambda i: (0, 0))
    return pl.pallas_call(
        functools.partial(_attend_kernel, heads=heads, bq=bq, bk=bk),
        grid=(s // bq,),
        in_specs=[rows(HALF), rows(HALF), full(HALF), full(HALF), rows(width), full(width), full(width)],
        out_specs=[rows(width), pl.BlockSpec((heads, bq), lambda i: (0, i)), rows(width), full(width)],
        scratch_shapes=[pltpu.VMEM((heads, bq), F32), pltpu.VMEM((heads, HEAD + 8, bq), F32), pltpu.VMEM((bk, STRIP), jnp.int32)],
        out_shape=[jax.ShapeDtypeStruct((s, width), BF), jax.ShapeDtypeStruct((heads, s), F32), jax.ShapeDtypeStruct((s, width), BF),
                   jax.ShapeDtypeStruct((s, width), BF)],
        compiler_params=pltpu.CompilerParams(dimension_semantics=("arbitrary",), vmem_limit_bytes=VMEM),
        cost_estimate=pl.CostEstimate(flops=6 * s * s * width, transcendentals=heads * s * s, bytes_accessed=14 * s * width),
    )(cos, sin, cos, sin, q, k, v)


def _attend_bwd_kernel(cq_ref, sq_ref, ck_ref, sk_ref, q_ref, k_ref, v_ref, o_ref, do_ref, lse_ref, dq_ref, dk_ref, dv_ref, dq_s, dk_s, dv_s, gap_s,
                       *, heads, bq, bk):
    iq = pl.program_id(1)
    sk = k_ref.shape[0]
    scale = HEAD**-0.5
    e = scale * LOG2E
    pieces = [(i, at) for i in range(heads) for at in range(0, bq, STRIP)]
    head = lambda i: slice(i * HEAD, (i + 1) * HEAD)

    @pl.when(iq == 0)
    def _():
        gap_s[...] = lax.broadcasted_iota(jnp.int32, (bk, STRIP), 1) - lax.broadcasted_iota(jnp.int32, (bk, STRIP), 0)
        dk_s[...] = jnp.zeros_like(dk_s)
        dv_s[...] = jnp.zeros_like(dv_s)

    dq_s[...] = jnp.zeros_like(dq_s)
    lses = [lse_ref[0, i : i + 1, :] * LOG2E for i in range(heads)]
    deltas = [(do_ref[:, head(i)].astype(F32) * o_ref[:, head(i)].astype(F32)).T.sum(axis=0, keepdims=True) for i in range(heads)]

    def block(j, pieces, diagonal):
        here = pl.ds(j * bk, bk)
        qs = [q_ref[at : at + STRIP, head(i)] for i, at in pieces]
        dos = [do_ref[at : at + STRIP, head(i)] for i, at in pieces]
        scores = [_dot(k_ref[here, head(i)], x, 1, 1) for (i, _), x in zip(pieces, qs)]
        dps = [_dot(v_ref[here, head(i)], x, 1, 1) for (i, _), x in zip(pieces, dos)]
        ok = gap_s[...] >= 0
        for n, (i, at) in enumerate(pieces):
            p = jnp.exp2(scores[n] * e - lses[i][:, at : at + STRIP])
            if at == diagonal:
                p = jnp.where(ok, p, 0.0)
            ds = (p * (dps[n] - deltas[i][:, at : at + STRIP])).astype(BF)
            dv_s[i, here, :] += _dot(p.astype(BF), dos[n], 1, 0)
            dk_s[i, here, :] += _dot(ds, qs[n], 1, 0)
            dq_s[i, :, at : at + STRIP] += _dot(k_ref[here, head(i)].T, ds, 1, 0)

    whole = iq * (bq // bk)
    lax.fori_loop(0, whole, lambda j, _: block(j, pieces, None), None)
    for at in range(0, bq, bk):
        block(whole + at // bk, [p for p in pieces if p[1] >= at], at)
    for i in range(heads):
        dq_ref[:, head(i)] = _turn_back((dq_s[i] * scale).T.astype(BF), cq_ref[...], sq_ref[...])

    @pl.when(iq == pl.num_programs(1) - 1)
    def _():
        def finish(n, _):
            at = pl.ds(n * 256, 256)
            for i in range(heads):
                dk_ref[at, head(i)] = _turn_back((dk_s[i, at, :] * scale).astype(BF), ck_ref[at, :], sk_ref[at, :])
                dv_ref[at, head(i)] = dv_s[i, at, :].astype(BF)

        lax.fori_loop(0, sk // 256, finish, None)


def attend_bwd(q, k, v, o, do, lse, cos, sin):
    s, width = q.shape
    heads, bq, bk = 2, 1024, STRIP
    w = heads * HEAD
    lse = lse.reshape(width // w, heads, s)
    rows = pl.BlockSpec((bq, w), lambda h, i: (i, h))
    full = pl.BlockSpec((s, w), lambda h, i: (0, h))
    table, tables = pl.BlockSpec((bq, HALF), lambda h, i: (i, 0)), pl.BlockSpec((s, HALF), lambda h, i: (0, 0), pipeline_mode=pl.Buffered(1))
    like = jax.ShapeDtypeStruct((s, width), BF)
    return pl.pallas_call(
        functools.partial(_attend_bwd_kernel, heads=heads, bq=bq, bk=bk),
        grid=(width // w, s // bq),
        in_specs=[table, table, tables, tables, rows, full, full, rows, rows, pl.BlockSpec((1, heads, bq), lambda h, i: (h, 0, i))],
        out_specs=[rows, full, full],
        scratch_shapes=[pltpu.VMEM((heads, HEAD, bq), F32), pltpu.VMEM((heads, s, HEAD), F32), pltpu.VMEM((heads, s, HEAD), F32),
                        pltpu.VMEM((bk, STRIP), jnp.int32)],
        out_shape=[like, like, like],
        compiler_params=pltpu.CompilerParams(dimension_semantics=("arbitrary", "arbitrary"), vmem_limit_bytes=63 * 2**20),
        cost_estimate=pl.CostEstimate(flops=12 * s * s * width, transcendentals=width // HEAD * s * s, bytes_accessed=16 * s * width),
    )(cos, sin, cos, sin, q, k, v, o, do, lse)


def matmul(a, w):
    return jnp.dot(a, w, preferred_element_type=F32).astype(BF)


def scale_of(wide):
    return lax.rsqrt(jnp.mean(wide**2, -1, keepdims=True) + 1e-6)


def normed(h):
    wide = h.astype(F32)
    return (wide * scale_of(wide)).astype(BF)


def norm_bwd(h, dn, dh):
    wide, dn = h.astype(F32), dn.astype(F32)
    s = scale_of(wide)
    mean = jnp.mean(wide * dn, -1, keepdims=True)
    return (dh.astype(F32) + s * (dn - wide * (s * s * mean))).astype(BF)


ROWS = 256
TILE = 512


def _strips(s):
    return [slice(at, at + ROWS) for at in range(0, s, ROWS)]


def _slopes(gate, up, dact):
    sig = jax.nn.sigmoid(gate)
    dact = dact.astype(BF).astype(F32)
    swish = gate * sig
    return (dact * up * (sig + swish * (1 - sig))).astype(BF), (dact * swish).astype(BF)


def _up_kernel(b_ref, wg_ref, wu_ref, gate_ref, up_ref, act_ref):
    for r in _strips(b_ref.shape[0]):
        gate, up = _dot(b_ref[r, :], wg_ref[...], 1, 0), _dot(b_ref[r, :], wu_ref[...], 1, 0)
        gate_ref[r, :] = gate
        up_ref[r, :] = up
        act_ref[r, :] = (gate * jax.nn.sigmoid(gate) * up).astype(BF)


def _slope_kernel(gate_ref, up_ref, dh_ref, wd_ref, dgate_ref, dup_ref):
    for r in _strips(dh_ref.shape[0]):
        dact = _dot(dh_ref[r, :], wd_ref[...], 1, 1)
        dgate_ref[r, :], dup_ref[r, :] = _slopes(gate_ref[r, :], up_ref[r, :], dact)


def _both_kernel(b_ref, wg_ref, wu_ref, dact_ref, act_ref, dgate_ref, dup_ref):
    for r in _strips(b_ref.shape[0]):
        gate, up = _dot(b_ref[r, :], wg_ref[...], 1, 0), _dot(b_ref[r, :], wu_ref[...], 1, 0)
        dact = dact_ref[r, :]
        act_ref[r, :] = (gate * jax.nn.sigmoid(gate) * up).astype(BF)
        dgate_ref[r, :], dup_ref[r, :] = _slopes(gate, up, dact)


def _back_kernel(*refs):
    pairs, (h_ref, dh_ref, out_ref) = refs[:-3], refs[-3:]
    for r in _strips(h_ref.shape[0]):
        dn = sum(_dot(g[r, :], w[...], 1, 1) for g, w in zip(pairs[::2], pairs[1::2]))
        out_ref[r, :] = norm_bwd(h_ref[r, :], dn.astype(BF), dh_ref[r, :])


def _ffn(kernel, arrays, kinds, outs, scratch, flops, exps):
    def spec(kind, a):
        if kind == "full":
            return pl.BlockSpec(a.shape, lambda n: (0, 0))
        if kind == "cols":
            return pl.BlockSpec((a.shape[0], TILE), lambda n: (0, n))
        number, way = kind
        if way == "out":
            return pl.BlockSpec((None, TILE, a.shape[2]), lambda n: (number, n, 0))
        return pl.BlockSpec((None, a.shape[1], TILE), lambda n: (number, 0, n))

    hidden = max(a.shape[-1] if kind == "cols" or kind[1] == "in" else 0 for kind, a in zip(kinds, arrays))
    return pl.pallas_call(
        kernel,
        grid=(hidden // TILE,),
        in_specs=[spec(kind, a) for kind, a in zip(kinds, arrays)],
        out_specs=[spec(kind, o) for kind, o in outs],
        out_shape=[o for _, o in outs],
        scratch_shapes=scratch,
        compiler_params=pltpu.CompilerParams(dimension_semantics=("arbitrary",), vmem_limit_bytes=VMEM),
        cost_estimate=pl.CostEstimate(flops=flops, transcendentals=exps, bytes_accessed=sum(o.size * o.dtype.itemsize for _, o in outs) * 2),
    )(*arrays)


def ffn_up(b, wide):
    s, d, f = *b.shape, wide.shape[2]
    like = lambda t: ("cols", jax.ShapeDtypeStruct((s, f), t))
    return _ffn(_up_kernel, [b, wide, wide], ["full", (0, "in"), (1, "in")], [like(F32), like(F32), like(BF)], [], 4 * s * d * f, s * f)


def ffn_slope(gate, up, dh, down, number):
    s, d, f = *dh.shape, gate.shape[1]
    like = ("cols", jax.ShapeDtypeStruct((s, f), BF))
    return _ffn(_slope_kernel, [gate, up, dh, down], ["cols", "cols", "full", (number, "out")], [like, like], [], 2 * s * d * f, s * f)


def ffn_both(b, wide, dact):
    s, d, f = *b.shape, wide.shape[2]
    like = ("cols", jax.ShapeDtypeStruct((s, f), BF))
    return _ffn(_both_kernel, [b, wide, wide, dact], ["full", (0, "in"), (1, "in"), "cols"], [like] * 3, [], 4 * s * d * f, s * f)


def norm_back(pairs, h, dh):
    s, d = h.shape
    rows = lambda a: pl.BlockSpec((2 * ROWS, a.shape[1]), lambda i: (i, 0))
    arrays, specs = [], []
    for g, (stack, number) in pairs:
        arrays += [g, stack]
        specs += [rows(g), pl.BlockSpec((None, *stack.shape[1:]), lambda i, number=number: (number, 0, 0), pipeline_mode=pl.Buffered(1))]
    flops = sum(2 * s * d * g.shape[1] for g, _ in pairs)
    return pl.pallas_call(
        _back_kernel,
        grid=(s // (2 * ROWS),),
        in_specs=[*specs, rows(h), rows(dh)],
        out_specs=rows(h),
        out_shape=jax.ShapeDtypeStruct((s, d), BF),
        compiler_params=pltpu.CompilerParams(dimension_semantics=("arbitrary",), vmem_limit_bytes=VMEM),
        cost_estimate=pl.CostEstimate(flops=flops, transcendentals=0, bytes_accessed=6 * s * d + flops // d),
    )(*arrays, h, dh)


def solution(mesh):
    n = mesh.shape["dp"]

    def gather(blocks):
        return lax.all_gather(jnp.stack(blocks), "dp", axis=1, tiled=True)

    class Scatter:
        def __init__(self, *dws):
            rows = dws[0].shape[0] // n
            self.own = [dw.reshape(n // 2, 2, rows, dw.shape[1]) for dw in dws]
            self.widths = [dw.shape[1] for dw in dws]
            self.stage, self.got, self.half = 0, None, None

        def term(self, chip):
            core = lax.axis_index("dp") & 1
            own = [lax.dynamic_slice(o, (chip, core, 0, 0), (1, 1, *o.shape[2:]))[0, 0] for o in self.own]
            got = lax.dynamic_index_in_dim(self.half, chip, 0, False)
            return jnp.concatenate(own, -1).astype(F32) + got.astype(F32)

        def outs(self):
            me = lax.axis_index("dp")
            if self.stage == 0:
                return [jnp.concatenate([lax.dynamic_index_in_dim(o, 1 - (me & 1), 1, False) for o in self.own], -1)]
            return [self.term((me >> 1) ^ m).astype(BF) for m in range(1, n // 2)]

        def send(self, outs):
            masks = [1] if self.stage == 0 else [2 * m for m in range(1, n // 2)]
            self.got = [lax.ppermute(o, "dp", [(i, i ^ mask) for i in range(n)]) for o, mask in zip(outs, masks)]

        def take(self):
            if self.stage == 0:
                self.half = self.got[0]
            else:
                self.others = self.got
            self.got = None
            self.stage += 1

        def result(self):
            while self.stage < 2:
                if self.got is None:
                    self.send(self.outs())
                self.take()
            total = self.term(lax.axis_index("dp") >> 1)
            for o in self.others:
                total += o.astype(F32)
            total, out, at = total.astype(BF), [], 0
            for w in self.widths:
                out.append(total[:, at : at + w])
                at += w
            return out

    class Offloaded:
        def __init__(self, blocks):
            block = jnp.stack(blocks) if len(blocks) > 1 else blocks[0]
            self.mib = block.size * 2 / 2**20
            self.got = lax.psum_scatter(block, "dp", scatter_dimension=block.ndim - 2, tiled=True)

        def parts(self):
            return list(self.got) if self.got.ndim == 3 else [self.got]

    class Line:
        def __init__(self):
            self.now, self.free, self.active, self.last = 0.0, [0.0, 0.0], [], None
            self.queue, self.queue_free = [], 0.0

        def step(self, took, *operands):
            self.now += took
            due = [s for s in self.active if s.got is not None and s.ready <= self.now]
            back = [o for o in self.queue if o.ready <= self.now]
            self.queue = [o for o in self.queue if o not in back]
            operands, _, gots, whole = lax.optimization_barrier((operands, self.last, [s.got for s in due], [o.got for o in back]))
            for o, got in zip(back, whole):
                o.got = got
            for s, got in zip(due, gots):
                s.got = got
                s.take()
            idle = [s for s in self.active if s.got is None and s.stage < 2]
            outs = [s.outs() for s in idle]
            operands, outs = lax.optimization_barrier((operands, outs))
            for s, out in zip(idle, outs):
                s.send(out)
                mib = out[0].size * 2 / 2**20
                begin = max(self.now, self.free[s.stage])
                s.ready = begin + (120 * mib if s.stage else 2.1 * mib) + 4
                self.free[s.stage] = s.ready
            return operands if len(operands) > 1 else operands[0]

        def flush(self):
            late = [s for s in self.active if s.got is not None]
            self.last, gots = lax.optimization_barrier((self.last, [s.got for s in late]))
            for s, got in zip(late, gots):
                s.got = got
            return self.last

        def done(self, result):
            self.last = result
            return result

        def scatter(self, *dws):
            self.active.append(Scatter(*dws))
            return self.active[-1]

        def offload(self, *blocks):
            o = Offloaded(blocks)
            o.ready = self.queue_free = max(self.now, self.queue_free) + 75 + 6.2 * o.mib
            self.queue.append(o)
            return o

    def step(x, dy, wq, wk, wv, wo, w_gate, w_up, w_down):
        h, dh = x[0], dy[0]
        s = h.shape[0]
        angle = jnp.arange(s, dtype=F32)[:, None] * THETA ** (-jnp.arange(HALF, dtype=F32) / HALF)
        cos, sin = jnp.cos(angle), jnp.sin(angle)

        small = [None, None]
        wide = [None, None]
        small[0] = gather([wq[0], wk[0], wv[0], wo[0]])
        wide[0] = gather([w_gate[0], w_up[0]])
        down = gather([w_down[0], w_down[1]])
        small[1] = gather([wq[1], wk[1], wv[1], wo[1]])
        wide[1] = gather([w_gate[1], w_up[1]])

        kept = []
        for l in range(2):
            a = normed(h)
            q, k, v = (matmul(a, small[l][i]) for i in range(3))
            o, lse, q, k = attend(q, k, v, cos, sin)
            h2 = h + matmul(o, small[l][3])
            b = normed(h2)
            if l == 0:
                gate, up, act = ffn_up(b, wide[l])
                kept.append((h, a, q, k, v, o, lse, h2, b, gate, up, act))
                h = h2 + matmul(act, down[l])
                h, dh_in = lax.optimization_barrier((h, dh))
                dact = matmul(dh_in, down[1].T)
                h, dact = lax.optimization_barrier((h, dact))
        act, dgate, dup = ffn_both(b, wide[1], dact)
        kept.append((h, a, q, k, v, o, lse, h2, b, None, None, act))

        grads = [None, None]
        line = Line()
        for l in (1, 0):
            h, a, q, k, v, o, lse, h2, b, gate, up, act = kept[l]
            big = line.offload if l in SLOW else line.scatter
            if l == 0:
                dh_in = line.step(6, dh)
                dgate, dup = ffn_slope(gate, up, dh_in, down, 0)
            line.done((dgate, dup))
            act, dh_in = line.step(40, act, dh)
            g_down = big(line.done(matmul(act.T, dh_in)))
            b1, dgate = line.step(26, b, dgate)
            g_gate = big(line.done(matmul(b1.T, dgate)))
            b1, dup = line.step(21, b, dup)
            g_up = big(line.done(matmul(b1.T, dup)))
            dgate = line.step(21, dgate)
            dh2 = line.done(norm_back([(dgate, (wide[l], 0)), (dup, (wide[l], 1))], h2, dh))
            dh_in = line.step(45, dh2)
            do = line.done(matmul(dh_in, small[l][3].T))
            do = line.step(8, do)
            dq, dk, dv = line.done(attend_bwd(q, k, v, o, do, lse, cos, sin))
            a1, dq = line.step(47, a, dq)
            g_q = line.done(matmul(a1.T, dq))
            a1, dk = line.step(6, a, dk)
            g_k = line.done(matmul(a1.T, dk))
            if l not in SLOW:
                few = [line.scatter(g_q, g_k)]
            a1, dv = line.step(6, a, dv)
            g_v = line.done(matmul(a1.T, dv))
            o1, dh_in = line.step(6, o, dh2)
            g_o = line.done(matmul(o1.T, dh_in))
            if l in SLOW:
                few = [line.offload(g_q, g_k, g_v, g_o)]
                dq = line.step(6, dq)
            else:
                few.append(line.scatter(g_v, g_o))
                dq = line.step(6, dq)
                dq = line.step(9, dq)
            dh = line.done(norm_back([(dq, (small[l], 0)), (dk, (small[l], 1)), (dv, (small[l], 2))], h, dh2))
            line.now += 25
            grads[l] = [*few, g_gate, g_up, g_down]
        dh = line.flush()
        grads = [[t for g in gs for t in (g.result() if isinstance(g, Scatter) else g.parts())] for gs in grads]
        return (dh[None], *(jnp.stack([grads[0][i], grads[1][i]]) for i in range(7)))

    states, cut = P(("rep", "dp"), None, None), P(None, "dp", None)
    return jax.shard_map(
        step,
        mesh=mesh,
        in_specs=(states, states) + (cut,) * 7,
        out_specs=(states,) + (P("rep", "dp", None),) * 7,
        check_vma=False,
    )
```
